32 devices in a mesh: gx: 16 (over z, y, x), gy: 2 (over core).
Axes of the slice: x: 2, y: 2, z: 4, core: 2. Of those that a mesh axis runs over, the one named last changes fastest.
Arguments:
- operator: float32 [243, 32768], P(None, ('gx', 'gy')), may hold values from -0.6 to 10.6
- basis_u: float32 [144, 32768], P(None, ('gx', 'gy')), may hold values from -6 to 6
- basis_c: float32 [144, 32768], P(None, ('gx', 'gy')), may hold values from -6 to 6
- right_side: float32 [3, 32768], P(None, ('gx', 'gy')), may hold values from -16 to 16
- new_rows: int32 [32768], P(('gx', 'gy')), may hold values from 0 to 32767, as said below
Outputs:
- solution: float32 [3, 32768], P(None, ('gx', 'gy'))
- residual: float32 [3, 32768], P(None, ('gx', 'gy'))
The draws below stay inside these ranges and needn't reach their ends.
Inputs may be any that keep to these rules, and one draw needn't show every extreme that they name: `new_rows`: each block row gets one new index (a permutation). Each device sends 0 to 64 of its old rows to each device, and each device both sends exactly 64 rows to some peer and receives exactly 64 rows from some peer.
All inputs are finite; a program needn't handle non-finite values.
Results may differ from the reference program's by a relative error of at most 0.0003.
Values sent between devices are 32-bit elements; how exact they have to be, the bound alone decides.
A program may use at most 64 MiB of HBM per device.

```python
import jax
import jax.numpy as jnp
from jax import lax

CX = 1
CY = 8
CZ = 128
K = 48
ROWS_DEV = 1024
PEERS = 32
ROWS = 32768
N_GX = 16
N_GY = 2


def c_values(key):
    values = jnp.clip(jax.random.normal(jax.random.fold_in(key, 11), (3 * K, ROWS), jnp.float32), -6.0, 6.0)
    return values


def draw_basis_c(key, part):
    return c_values(key)


def draw_right_side(key, part):
    values = c_values(key).reshape(3, K, ROWS)
    weights = jax.random.normal(jax.random.fold_in(key, 13), (K,), jnp.float32) / jnp.sqrt(1.0 * K)
    along = jnp.einsum('amp,m->ap', values, weights)
    owner = (draw_new_rows(key, part) // ROWS_DEV).astype(jnp.float32)
    place = owner / (1.0 * (PEERS - 1))
    noise = jax.random.normal(jax.random.fold_in(key, 12), (3, ROWS), jnp.float32)
    rising = 1.0 + 4.0 * place
    return jnp.clip(noise * rising[None, :] + along, -16.0, 16.0)


def draw_operator(key, part):
    off = jnp.clip(0.1 * jax.random.normal(jax.random.fold_in(key, 21), (27, 3, 3, ROWS), jnp.float32), -0.6, 0.6)
    diag = 6.0 + 4.0 * jax.random.uniform(jax.random.fold_in(key, 22), (3, ROWS), jnp.float32)
    eye = jnp.eye(3, dtype=jnp.float32)
    off = off.at[13].add(eye[:, :, None] * diag[:, None, :])
    return off.reshape(243, ROWS)


def draw_new_rows(key, part):
    peers = PEERS
    rows = ROWS_DEV
    base = rows // peers
    half = jax.random.randint(jax.random.fold_in(key, 31), (peers // 2,), -base, base + 1)
    half = half.at[0].set(base)
    sizes = base + jnp.concatenate([half, -half])
    sigma = jax.random.permutation(jax.random.fold_in(key, 32), peers)
    tau = jax.random.permutation(jax.random.fold_in(key, 33), peers)
    counts = sizes[(sigma[:, None] + tau[None, :]) % peers]
    offsets = jnp.cumsum(counts, 0) - counts
    ends = jnp.cumsum(counts, 1)
    starts = ends - counts
    keys = jax.random.split(jax.random.fold_in(key, 34), peers)
    orders = jax.vmap(lambda k: jax.random.permutation(k, rows))(keys)
    places = jnp.arange(rows, dtype=jnp.int32)

    def one_source(order, end_row, start_row, offset_row):
        target = jnp.searchsorted(end_row, places, side='right').astype(jnp.int32)
        newer = target * rows + offset_row[target] + places - start_row[target]
        return jnp.zeros((rows,), jnp.int32).at[order].set(newer.astype(jnp.int32))
    table = jax.vmap(one_source)(orders, ends, starts, offsets)
    return table.reshape(peers * rows).astype(jnp.int32)


def level_of(key, extent, shards, smallest, high):
    loudness = 1.0
    for dim, blocks in shards:
        draws = jax.random.uniform(jax.random.fold_in(jax.random.fold_in(key, 6), dim), (blocks,), jnp.float32, smallest / len(shards), high / len(shards))
        loudness = loudness * jnp.repeat(jnp.exp(draws), extent[dim] // blocks).reshape((-1,) + (1,) * (len(extent) - 1 - dim))
    return loudness


def gaussian(key, shape, scale, reach, cuts=(), kind=jnp.bfloat16):
    result = jax.random.normal(key, shape, jnp.float32) * scale
    if len(cuts) > 0:
        result = level_of(key, shape, cuts, -0.22, 0.18) * result
    return jnp.clip(result, min=-reach, max=reach).astype(kind)


def setup_inputs(seed: int = 0) -> dict:
    key_of = jax.random.split(jax.random.key(seed), 6)
    return {
        "operator": draw_operator(jax.random.fold_in(key_of[5], 71), 0),
        "basis_u": gaussian(key_of[1], (3 * K, ROWS), 1.0, 6.0, ((1, 32),), jnp.float32),
        "basis_c": draw_basis_c(jax.random.fold_in(key_of[5], 71), 0),
        "right_side": draw_right_side(jax.random.fold_in(key_of[5], 71), 0),
        "new_rows": draw_new_rows(jax.random.fold_in(key_of[5], 71), 0),
    }


def to_grid(values):
    width = values.shape[0]
    shaped = values.reshape(width, N_GX, N_GY, CX, CY, CZ).transpose(0, 1, 3, 2, 4, 5)
    return shaped.reshape(width, N_GX * CX, N_GY * CY, CZ)

def to_rows(grid):
    width = grid.shape[0]
    shaped = grid.reshape(width, N_GX, CX, N_GY, CY, CZ).transpose(0, 1, 3, 2, 4, 5)
    return shaped.reshape(width, ROWS)

def stencil(coef, padded):
    size_x = padded.shape[1] - 2
    size_y = padded.shape[2] - 2
    size_z = padded.shape[3] - 2
    total = jnp.zeros((3, size_x, size_y, size_z), jnp.float32)
    for k in range(27):
        dx, dy, dz = (k // 9, k // 3 % 3, k % 3)
        moved = padded[:, dx:dx + size_x, dy:dy + size_y, dz:dz + size_z]
        total = total + lax.optimization_barrier(jnp.sum(coef[k] * moved[None], axis=1))
    return total

def apply_op(coef, vector):
    padded = jnp.pad(to_grid(vector), ((0, 0), (1, 1), (1, 1), (1, 1)))
    return to_rows(stencil(coef, padded))

def project(basis, vector):
    return jnp.einsum('amp,ap->m', basis, vector, precision=lax.Precision.HIGHEST)

def combine(basis, coeffs):
    return jnp.einsum('amp,m->ap', basis, coeffs, precision=lax.Precision.HIGHEST)

def reference(operator, basis_u, basis_c, right_side, new_rows):
    payload = jnp.concatenate([operator, basis_u, basis_c, right_side], 0)
    moved = jnp.zeros_like(payload).at[:, new_rows].set(payload)
    coef = to_grid(moved[:243]).reshape(27, 3, 3, N_GX * CX, N_GY * CY, CZ)
    u = moved[243:243 + 3 * K].reshape(3, K, ROWS)
    c = moved[243 + 3 * K:243 + 6 * K].reshape(3, K, ROWS)
    b = moved[243 + 6 * K:]
    gram = jnp.einsum('amp,anp->mn', c, c, precision=lax.Precision.HIGHEST)
    lower = jnp.linalg.cholesky(gram)
    lower_inv = jax.scipy.linalg.solve_triangular(lower, jnp.eye(K, dtype=jnp.float32), lower=True)
    cq = jnp.einsum('mn,anp->amp', lower_inv, c, precision=lax.Precision.HIGHEST)
    uq = jnp.einsum('mn,anp->amp', lower_inv, u, precision=lax.Precision.HIGHEST)
    start = project(cq, b)
    first_x = combine(uq, start)
    first_r = b - combine(cq, start)
    beta = jnp.sqrt(jnp.sum(first_r * first_r))
    vec_one = first_r / beta
    image = apply_op(coef, vec_one)
    proj_one = project(cq, image)
    h11 = jnp.sum(vec_one * image)
    rest = image - combine(cq, proj_one) - h11 * vec_one
    h21 = jnp.sqrt(jnp.sum(rest * rest))
    vec_two = rest / h21
    image = apply_op(coef, vec_two)
    proj_two = project(cq, image)
    h12 = jnp.sum(vec_one * image)
    h22 = jnp.sum(vec_two * image)
    rest = image - combine(cq, proj_two) - h12 * vec_one - h22 * vec_two
    h32 = jnp.sqrt(jnp.sum(rest * rest))
    m11 = h11 * h11 + h21 * h21
    m12 = h11 * h12 + h21 * h22
    m22 = h12 * h12 + h22 * h22 + h32 * h32
    g_one = beta * h11
    g_two = beta * h12
    determ = m11 * m22 - m12 * m12
    y_one = (m22 * g_one - m12 * g_two) / determ
    y_two = (m11 * g_two - m12 * g_one) / determ
    solution = first_x + y_one * vec_one + y_two * vec_two - combine(uq, y_one * proj_one + y_two * proj_two)
    residual = b - apply_op(coef, solution)
    return (solution, residual)
```

```python
import functools

import jax
import jax.numpy as jnp
from jax import lax
from jax.experimental import pallas as pl
from jax.experimental.pallas import tpu as pltpu
from jax.sharding import PartitionSpec as P

CY = 8
CZ = 128
F32 = jnp.float32
BF16 = jnp.bfloat16
HIGH = lax.Precision.HIGHEST
NT = (((1,), (1,)), ((), ()))


def round_up(n, m):
    return (n + m - 1) // m * m


class Plan:
    def __init__(self, nx, ny, rows, op_rows, basis_rows):
        self.nx, self.ny, self.rows = nx, ny, rows
        self.peers = nx * ny
        self.k = basis_rows // 3
        self.op_rows, self.basis_rows = op_rows, basis_rows
        self.cap = 2 * rows // self.peers
        self.fold = CZ // self.cap
        self.c0 = round_up(op_rows, 8)
        self.b0 = self.c0 + basis_rows
        self.tag = self.b0 + 3
        self.part = round_up(-(-(self.tag + 1) // self.fold), 8)
        self.width = round_up(self.part * self.fold, 16)
        self.part = self.width // self.fold
        self.nblk = 2 * rows // 256
        self.per_blk = 2 * self.fold
        self.tiles = (self.k + 2 + 7) // 8
        self.stride = max(1, self.peers // 8)


def kernel(
    pn, op_ref, u_ref, c_ref, b_ref, rcol_ref, rrow_ref, sol_ref, res_ref,
    pay, hl, slot, ohp, xs, snd, got, xhl, oht, acc, new, uv,
    gpart, grs, gsnd, gfull, gm, ginv,
    hsnd, hrcv, mred, rsnd, rrcv, ulhs, usnd, urcv,
    bulk_s, bulk_r, rs_s, rs_r, ag_s, ag_r, h_s, h_r, red_s, red_r, u_s, u_r,
):
    gx, gy = lax.axis_index("gx"), lax.axis_index("gy")
    me = gx * pn.ny + gy
    peers, rows, k = pn.peers, pn.rows, pn.k

    def dev(p):
        return {"gx": lax.div(p, pn.ny), "gy": lax.rem(p, pn.ny)}

    def remote(src, dst, ssem, rsem, p):
        return pltpu.make_async_remote_copy(
            src_ref=src, dst_ref=dst, send_sem=ssem, recv_sem=rsem,
            device_id=dev(p), device_id_type=pl.DeviceIdType.MESH,
        )

    def others(body):
        def step(d, _):
            body(lax.rem(me + d, peers))
            return 0
        lax.fori_loop(1, peers, step, 0)

    barrier = pltpu.get_barrier_semaphore()
    others(lambda p: pl.semaphore_signal(
        barrier, inc=1, device_id=dev(p), device_id_type=pl.DeviceIdType.MESH))

    pay[0 : pn.op_rows, :] = op_ref[...]
    pay[pn.op_rows : pn.c0, :] = jnp.zeros((pn.c0 - pn.op_rows, rows), F32)
    pay[pn.c0 : pn.b0, :] = c_ref[...]
    pay[pn.b0 : pn.width, :] = jnp.zeros((pn.width - pn.b0, rows), F32)
    pay[pn.b0 : pn.tag, :] = b_ref[...]
    shift = rows.bit_length() - 1
    local = lax.bitwise_and(rrow_ref[...], rows - 1) + 1
    pay[pn.tag : pn.tag + 1, :] = local.astype(F32)

    gpart[...] = jnp.zeros(gpart.shape, F32)
    gram = jnp.zeros((k, k), F32)
    raw = jnp.zeros((1, k), F32)
    b8 = pay[pn.b0 : pn.b0 + 8, :]
    for a in range(3):
        ca = pay[pn.c0 + a * k : pn.c0 + (a + 1) * k, :]
        gram = gram + lax.dot_general(ca, ca, NT, precision=HIGH, preferred_element_type=F32)
        raw = raw + lax.dot_general(b8, ca, NT, precision=HIGH, preferred_element_type=F32)[a : a + 1]
    b3 = pay[pn.b0 : pn.tag, :]
    bb = jnp.sum(jnp.sum(b3 * b3, axis=1, keepdims=True), axis=0, keepdims=True)
    gpart[0:k, 0:k] = gram
    gpart[k : k + 1, 0:k] = raw
    gpart[k + 1 : k + 2, :] = jnp.broadcast_to(bb, (1, CZ))

    pl.semaphore_wait(barrier, peers - 1)

    def tile(t):
        return pl.ds(pl.multiple_of(t * 8, 8), 8)

    def rs_send(t, _):
        own = t * pn.stride

        @pl.when(me != own)
        def _():
            remote(gpart.at[tile(t), :], grs.at[me], rs_s.at[t], rs_r.at[me], own).start()
        return 0

    lax.fori_loop(0, pn.tiles, rs_send, 0)

    trow = lax.shift_right_logical(rrow_ref[...], shift)
    jrow = lax.broadcasted_iota(jnp.int32, (CZ, rows), 1)
    irow = lax.broadcasted_iota(jnp.int32, (CZ, rows), 0)

    def slots(i, _):
        at = pl.ds(pl.multiple_of(i * CZ, CZ), CZ)
        tc = lax.shift_right_logical(rcol_ref[at, :], shift)
        before = jnp.logical_and(tc == trow, jrow < irow + i * CZ)
        rank = jnp.sum(jnp.where(before, 1.0, 0.0), axis=1, keepdims=True)
        slot[at, :] = jnp.broadcast_to(tc * pn.cap + rank.astype(jnp.int32), (CZ, CZ))
        return 0

    lax.fori_loop(0, rows // CZ, slots, 0)
    full = pay[...]
    hi = full.astype(BF16)
    hl[0 : pn.width, :] = hi
    hl[pn.width :, :] = (full - hi.astype(F32)).astype(BF16)

    mine = lax.div(me, pn.stride)
    owner = jnp.logical_and(lax.rem(me, pn.stride) == 0, mine < pn.tiles)

    @pl.when(owner)
    def _():
        grs[me] = gpart[tile(mine), :]
        others(lambda p: remote(gpart.at[tile(0), :], grs.at[p], rs_s.at[0], rs_r.at[p], p).wait_recv())
        total = jnp.sum(grs[...], axis=0)
        gsnd[...] = total
        gfull[mine] = total
        others(lambda p: remote(gsnd, gfull.at[mine], ag_s.at[p], ag_r.at[mine], p).start())

    lane = lax.broadcasted_iota(jnp.int32, (1, CZ), 1)
    block = lax.div(me, pn.per_blk)

    def spread(parts, q):
        out = None
        for j, value in enumerate(parts):
            amount = (j - q) * pn.cap % CZ
            moved = pltpu.roll(value, amount, 1) if amount else value
            out = moved if out is None else jnp.where(lane >= j * pn.cap, moved, out)
        return out

    def pack(it, _):
        gb = lax.rem(block + it, pn.nblk)
        for half in range(2):
            ids = lane + (gb * 256 + half * CZ)
            ohp[gb, :, half * CZ : (half + 1) * CZ] = jnp.where(slot[...] == ids, 1.0, 0.0).astype(BF16)
        oh = ohp[gb]
        xs[...] = jnp.dot(hl[0 : pn.width, :], oh, preferred_element_type=F32)
        xs[...] += jnp.dot(hl[pn.width :, :], oh, preferred_element_type=F32)
        for half in range(2):
            parts = [xs[j * pn.part : (j + 1) * pn.part, half * CZ : (half + 1) * CZ] for j in range(pn.fold)]
            for q in range(pn.fold):
                p = gb * pn.per_blk + half * pn.fold + q
                packet = spread(parts, q)

                @pl.when(p == me)
                def _():
                    got[p] = packet

                @pl.when(p != me)
                def _():
                    snd[p] = packet
                    remote(snd.at[p], got.at[me], bulk_s.at[p], bulk_r.at[me], p).start()
        return 0

    lax.fori_loop(0, pn.nblk, pack, 0)

    for y in range(CY):
        uv[pl.ds(y, pn.basis_rows, stride=CY), :] = u_ref[:, y * CZ : (y + 1) * CZ]
    mred[...] = jnp.zeros(mred.shape, F32)
    ginv[...] = jnp.zeros(ginv.shape, F32)

    def ag_wait(t, _):
        own = t * pn.stride

        @pl.when(me != own)
        def _():
            remote(gsnd, gfull.at[t], ag_s.at[0], ag_r.at[t], own).wait_recv()
        return 0

    lax.fori_loop(0, pn.tiles, ag_wait, 0)
    sums = gfull[...].reshape(pn.tiles * 8, CZ)
    gm[...] = sums[0:k]
    sub_k = lax.broadcasted_iota(jnp.int32, (k, 1), 0)

    def sweep(i, _):
        m = gm[...]
        row = gm[pl.ds(i, 1), :]
        at = lane == i
        col = jnp.sum(jnp.where(at, m, 0.0), axis=1, keepdims=True)
        pivot = jnp.sum(jnp.where(at, row, 0.0), axis=1, keepdims=True)
        scaled = jnp.where(at, 1.0, row) / pivot
        inner = jnp.where(at, 0.0, m) - col * scaled
        gm[...] = jnp.where(sub_k == i, scaled, inner)
        return 0

    lax.fori_loop(0, k, sweep, 0)
    ginv[0:k, :] = gm[...]

    def solve(p):
        return jnp.dot(p, ginv[...], precision=HIGH, preferred_element_type=F32)

    def bdot(p, z):
        return jnp.sum(jnp.where(lane < k, p * z, 0.0), axis=1, keepdims=True)

    s_row = jnp.broadcast_to(sums[k : k + 1, :], (8, CZ))
    bb_all = jnp.broadcast_to(sums[k + 1 : k + 2, 0:1], (8, 1))
    z0 = solve(s_row)
    beta = jnp.sqrt(bb_all - bdot(s_row, z0))

    acc[...] = jnp.zeros(acc.shape, F32)
    sub_r = lax.broadcasted_iota(jnp.int32, (rows, 1), 0).astype(F32) + 1.0

    def unpack(it, _):
        gb = lax.rem(block - it + pn.nblk, pn.nblk)
        for half in range(2):
            values = []
            for q in range(pn.fold):
                p = gb * pn.per_blk + half * pn.fold + q

                @pl.when(p != me)
                def _():
                    remote(snd.at[p], got.at[p], bulk_s.at[p], bulk_r.at[p], p).wait_recv()
            for q in range(pn.fold):
                values.append(got[gb * pn.per_blk + half * pn.fold + q])
            for j in range(pn.fold):
                xs[j * pn.part : (j + 1) * pn.part, half * CZ : (half + 1) * CZ] = spread(values, j)
            tags = xs[pn.tag : pn.tag + 1, half * CZ : (half + 1) * CZ]
            oht[gb, :, half * CZ : (half + 1) * CZ] = jnp.where(sub_r == tags, 1.0, 0.0).astype(BF16)
        x = xs[...]
        xh = x.astype(BF16)
        xhl[0 : pn.width, :] = xh
        xhl[pn.width :, :] = (x - xh.astype(F32)).astype(BF16)
        for n in range(rows // 256):
            at = slice(n * 256, (n + 1) * 256)
            o = oht[gb, at, :]
            acc[:, at] += lax.dot_general(xhl[0 : pn.width, :], o, NT, preferred_element_type=F32)
            acc[:, at] += lax.dot_general(xhl[pn.width :, :], o, NT, preferred_element_type=F32)
        return 0

    lax.fori_loop(0, pn.nblk, unpack, 0)
    for y in range(CY):
        new[pl.ds(y, pn.width, stride=CY), :] = acc[:, y * CZ : (y + 1) * CZ]

    def row(i):
        return new[i * CY : (i + 1) * CY, :]

    sub = lax.broadcasted_iota(jnp.int32, (CY, CZ), 0)
    lane8 = lax.broadcasted_iota(jnp.int32, (CY, CZ), 1)

    def combine(get, z):
        out = [jnp.zeros((CY, CZ), F32)] * 3
        for m in range(k):
            zb = jnp.broadcast_to(z[:, m : m + 1], (CY, CZ))
            for a in range(3):
                out[a] = out[a] + get(a * k + m) * zb
        return out

    def c_row(i):
        return row(pn.c0 + i)

    def u_row(i):
        return uv[i * CY : (i + 1) * CY, :]

    places = ((-1, 0), (1, 0), (0, 1), (-1, 1), (1, 1))

    def apply_op(phase, v):
        for b in range(3):
            hsnd[phase, b] = v[b]
        for j, (dx, oy) in enumerate(places):
            to = gx - dx
            target = to * pn.ny + (lax.rem(gy + oy, 2))

            @pl.when(jnp.logical_and(to >= 0, to < pn.nx))
            def _():
                remote(hsnd.at[phase], hrcv.at[phase, j], h_s.at[phase, j], h_r.at[phase, j], target).start()
        for j, (dx, oy) in enumerate(places):
            there = gx + dx
            source = there * pn.ny + (lax.rem(gy + oy, 2))
            valid = jnp.logical_and(there >= 0, there < pn.nx)

            @pl.when(valid)
            def _():
                remote(hsnd.at[phase], hrcv.at[phase, j], h_s.at[phase, j], h_r.at[phase, j], source).wait_recv()

            @pl.when(jnp.logical_not(valid))
            def _():
                hrcv[phase, j] = jnp.zeros((3, CY, CZ), F32)
        out = [jnp.zeros((CY, CZ), F32)] * 3
        for dx in (-1, 0, 1):
            for b in range(3):
                near = v[b] if dx == 0 else hrcv[phase, places.index((dx, 0)), b]
                side = hrcv[phase, places.index((dx, 1)), b]
                for dy in (-1, 0, 1):
                    if dy == 0:
                        moved = near
                    elif dy == -1:
                        edge = jnp.where(gy > 0, pltpu.roll(side, 1, 0), 0.0)
                        moved = jnp.where(sub == 0, edge, pltpu.roll(near, 1, 0))
                    else:
                        edge = jnp.where(gy == 0, pltpu.roll(side, CY - 1, 0), 0.0)
                        moved = jnp.where(sub == CY - 1, edge, pltpu.roll(near, CY - 1, 0))
                    for dz in (-1, 0, 1):
                        if dz == 0:
                            value = moved
                        elif dz == -1:
                            value = jnp.where(lane8 == 0, 0.0, pltpu.roll(moved, 1, 1))
                        else:
                            value = jnp.where(lane8 == CZ - 1, 0.0, pltpu.roll(moved, CZ - 1, 1))
                        kk = (dx + 1) * 9 + (dy + 1) * 3 + dz + 1
                        for a in range(3):
                            out[a] = out[a] + row((kk * 3 + a) * 3 + b) * value
        return out

    def put(i, value):
        mred[i : i + 1, :] = jnp.sum(value, axis=0, keepdims=True)

    def dot3(p, q):
        return p[0] * q[0] + p[1] * q[1] + p[2] * q[2]

    def sums_of(phase, image, vectors):
        for m in range(k):
            put(m, dot3([c_row(a * k + m) for a in range(3)], image))
        for i, vector in enumerate(vectors + [image]):
            put(k + i, dot3(vector, image))
        mine_row = lax.dot_general(jnp.ones((8, CZ), F32), mred[...], NT, precision=HIGH, preferred_element_type=F32)
        rsnd[phase] = mine_row
        rrcv[phase, me] = mine_row
        others(lambda p: remote(rsnd.at[phase], rrcv.at[phase, me], red_s.at[phase, p], red_r.at[phase, me], p).start())
        others(lambda p: remote(rsnd.at[phase], rrcv.at[phase, p], red_s.at[phase, p], red_r.at[phase, p], p).wait_recv())
        return jnp.sum(rrcv[phase], axis=0)

    load = [row(pn.b0 + a) for a in range(3)]
    part = combine(c_row, z0)
    v1 = [(load[a] - part[a]) / beta for a in range(3)]
    w = apply_op(0, v1)
    p1 = sums_of(0, w, [v1])
    z1 = solve(p1)
    h11, ww = p1[:, k : k + 1], p1[:, k + 1 : k + 2]
    h21 = jnp.sqrt(ww - bdot(p1, z1) - h11 * h11)
    part = combine(c_row, z1)
    v2 = [(w[a] - part[a] - h11 * v1[a]) / h21 for a in range(3)]
    w = apply_op(1, v2)
    p2 = sums_of(1, w, [v1, v2])
    z2 = solve(p2)
    h12, h22, ww = p2[:, k : k + 1], p2[:, k + 1 : k + 2], p2[:, k + 2 : k + 3]
    h32 = jnp.sqrt(ww - bdot(p2, z2) - h12 * h12 - h22 * h22)
    m11 = h11 * h11 + h21 * h21
    m12 = h11 * h12 + h21 * h22
    m22 = h12 * h12 + h22 * h22 + h32 * h32
    g_one, g_two = beta * h11, beta * h12
    determ = m11 * m22 - m12 * m12
    y_one = (m22 * g_one - m12 * g_two) / determ
    y_two = (m11 * g_two - m12 * g_one) / determ

    ut = combine(u_row, z0 - y_one * z1 - y_two * z2)
    for y in range(CY):
        tile_y = jnp.zeros((8, CZ), F32)
        for a in range(3):
            tile_y = jnp.where(sub == a, jnp.broadcast_to(ut[a][y : y + 1, :], (8, CZ)), tile_y)
        high = tile_y.astype(BF16).astype(F32)
        ulhs[0:8, y * CZ : (y + 1) * CZ] = high
        ulhs[8:16, y * CZ : (y + 1) * CZ] = tile_y - high
    ub = ulhs[...].astype(BF16)

    def upack(gb, _):
        d = jnp.dot(ub, ohp[gb], preferred_element_type=F32)
        d = d[0:8] + d[8:16]
        usnd[2 * gb] = d[:, :CZ]
        usnd[2 * gb + 1] = d[:, CZ:]
        return 0

    lax.fori_loop(0, pn.nblk, upack, 0)
    others(lambda p: remote(usnd.at[lax.div(p, pn.fold)], urcv.at[me], u_s.at[p], u_r.at[me], p).start())
    urcv[me] = usnd[lax.div(me, pn.fold)]
    others(lambda p: remote(usnd.at[0], urcv.at[p], u_s.at[p], u_r.at[p], p).wait_recv())
    place = lax.rem(me, pn.fold)

    def uunpack(gb, total):
        halves = []
        for half in range(2):
            out = None
            for q in range(pn.fold):
                tile_q = urcv[gb * pn.per_blk + half * pn.fold + q]
                if pn.fold > 1:
                    tile_q = pltpu.roll(tile_q, lax.rem((q - place) * pn.cap + CZ, CZ), 1)
                out = tile_q if out is None else jnp.where(lane >= q * pn.cap, tile_q, out)
            halves.append(out)
        x = jnp.concatenate(halves, axis=1)
        high = x.astype(BF16).astype(F32)
        x2 = jnp.concatenate([high, x - high], axis=0).astype(BF16)
        return total + lax.dot_general(x2, oht[gb], NT, preferred_element_type=F32)

    moved = lax.fori_loop(0, pn.nblk, uunpack, jnp.zeros((16, rows), F32))
    moved = moved[0:8] + moved[8:16]
    sol = []
    for a in range(3):
        value = jnp.zeros((CY, CZ), F32)
        for y in range(CY):
            line = jnp.broadcast_to(moved[a : a + 1, y * CZ : (y + 1) * CZ], (CY, CZ))
            value = jnp.where(sub == y, line, value)
        sol.append(value + y_one * v1[a] + y_two * v2[a])
        sol_ref[a] = sol[a]
    w = apply_op(2, sol)
    for a in range(3):
        res_ref[a] = row(pn.b0 + a) - w[a]

    def rs_done(t, _):
        own = t * pn.stride

        @pl.when(me != own)
        def _():
            remote(gpart.at[tile(t), :], grs.at[me], rs_s.at[t], rs_r.at[me], own).wait_send()
        return 0

    lax.fori_loop(0, pn.tiles, rs_done, 0)

    @pl.when(owner)
    def _():
        others(lambda p: remote(gsnd, gfull.at[mine], ag_s.at[p], ag_r.at[mine], p).wait_send())

    others(lambda p: remote(snd.at[p], got.at[me], bulk_s.at[p], bulk_r.at[me], p).wait_send())
    for phase in range(2):
        others(lambda p: remote(rsnd.at[phase], rrcv.at[phase, me], red_s.at[phase, p], red_r.at[phase, me], p).wait_send())
    others(lambda p: remote(usnd.at[lax.div(p, pn.fold)], urcv.at[me], u_s.at[p], u_r.at[me], p).wait_send())
    for phase in range(3):
        for j, (dx, oy) in enumerate(places):
            to = gx - dx
            target = to * pn.ny + (lax.rem(gy + oy, 2))

            @pl.when(jnp.logical_and(to >= 0, to < pn.nx))
            def _():
                remote(hsnd.at[phase], hrcv.at[phase, j], h_s.at[phase, j], h_r.at[phase, j], target).wait_send()


def body(nx, ny, operator, basis_u, basis_c, right_side, new_rows):
    rows = operator.shape[1]
    pn = Plan(nx, ny, rows, operator.shape[0], basis_u.shape[0])
    n = pn.peers
    vmem, dma = pltpu.VMEM, pltpu.SemaphoreType.DMA
    out = jax.ShapeDtypeStruct((3, CY, CZ), F32)
    whole = pl.BlockSpec(memory_space=pltpu.VMEM)
    sol, res = pl.pallas_call(
        functools.partial(kernel, pn),
        out_shape=(out, out),
        in_specs=[whole] * 6,
        out_specs=(whole, whole),
        scratch_shapes=[
            vmem((pn.width, rows), F32),
            vmem((2 * pn.width, rows), BF16),
            vmem((rows, CZ), jnp.int32),
            vmem((pn.nblk, rows, 256), BF16),
            vmem((pn.width, 256), F32),
            vmem((n, pn.part, CZ), F32),
            vmem((n, pn.part, CZ), F32),
            vmem((2 * pn.width, 256), BF16),
            vmem((pn.nblk, rows, 256), BF16),
            vmem((pn.width, rows), F32),
            vmem((pn.width * CY, CZ), F32),
            vmem((pn.basis_rows * CY, CZ), F32),
            vmem((pn.tiles * 8, CZ), F32),
            vmem((n, 8, CZ), F32),
            vmem((8, CZ), F32),
            vmem((pn.tiles, 8, CZ), F32),
            vmem((pn.k, CZ), F32),
            vmem((CZ, CZ), F32),
            vmem((3, 3, CY, CZ), F32),
            vmem((3, 5, 3, CY, CZ), F32),
            vmem((CZ, CZ), F32),
            vmem((2, 8, CZ), F32),
            vmem((2, n, 8, CZ), F32),
            vmem((16, rows), F32),
            vmem((2 * pn.nblk, 8, CZ), F32),
            vmem((n, 8, CZ), F32),
            dma((n,)), dma((n,)),
            dma((pn.tiles,)), dma((n,)),
            dma((n,)), dma((pn.tiles,)),
            dma((3, 5)), dma((3, 5)),
            dma((2, n)), dma((2, n)),
            dma((n,)), dma((n,)),
        ],
        compiler_params=pltpu.CompilerParams(
            collective_id=0, has_side_effects=True, vmem_limit_bytes=60 << 20
        ),
        name="solve",
    )(operator, basis_u, basis_c, right_side, new_rows.reshape(rows, 1), new_rows.reshape(1, rows))
    return sol.reshape(3, rows), res.reshape(3, rows)


def solution(mesh):
    split = P(None, ("gx", "gy"))
    return jax.shard_map(
        functools.partial(body, mesh.shape["gx"], mesh.shape["gy"]),
        mesh=mesh,
        in_specs=(split, split, split, split, P(("gx", "gy"))),
        out_specs=(split, split),
        check_vma=False,
    )
```

```python
import functools

import jax
import jax.numpy as jnp
from jax import lax
from jax.experimental import pallas as pl
from jax.experimental.pallas import tpu as pltpu
from jax.sharding import PartitionSpec as P

CY = 8
CZ = 128
F32 = jnp.float32
BF16 = jnp.bfloat16
HIGH = lax.Precision.HIGHEST
NT = (((1,), (1,)), ((), ()))


def round_up(n, m):
    return (n + m - 1) // m * m


class Plan:
    def __init__(self, nx, ny, rows, op_rows, basis_rows):
        self.nx, self.ny, self.rows = nx, ny, rows
        self.peers = nx * ny
        self.k = basis_rows // 3
        self.op_rows, self.basis_rows = op_rows, basis_rows
        self.cap = 2 * rows // self.peers
        self.fold = CZ // self.cap
        self.c0 = round_up(op_rows, 8)
        self.b0 = self.c0 + basis_rows
        self.tag = self.b0 + 3
        self.part = round_up(-(-(self.tag + 1) // self.fold), 8)
        self.width = round_up(self.part * self.fold, 16)
        self.part = self.width // self.fold
        self.nblk = 2 * rows // 256
        self.per_blk = 2 * self.fold
        self.tiles = (self.k + 2 + 7) // 8
        self.stride = max(1, self.peers // 8)


def kernel(
    pn, op_ref, u_ref, c_ref, b_ref, rrow_ref, sol_ref, res_ref,
    pay, hl, slot, ohp, xs, snd, got, xhl, oht, acc, new, uv,
    gpart, grs, gsnd, gfull, gm, ginv,
    hsnd, hrcv, mred, rsnd, rrcv, ulhs, usnd, urcv, utmp,
    bulk_s, bulk_r, rs_s, rs_r, ag_s, ag_r, h_s, h_r, red_s, red_r, u_s, u_r,
):
    gx, gy = lax.axis_index("gx"), lax.axis_index("gy")
    me = gx * pn.ny + gy
    peers, rows, k = pn.peers, pn.rows, pn.k

    def dev(p):
        return {"gx": lax.div(p, pn.ny), "gy": lax.rem(p, pn.ny)}

    def remote(src, dst, ssem, rsem, p):
        return pltpu.make_async_remote_copy(
            src_ref=src, dst_ref=dst, send_sem=ssem, recv_sem=rsem,
            device_id=dev(p), device_id_type=pl.DeviceIdType.MESH,
        )

    def others(body):
        def step(d, _):
            body(lax.rem(me + d, peers))
            return 0
        lax.fori_loop(1, peers, step, 0)

    barrier = pltpu.get_barrier_semaphore()
    others(lambda p: pl.semaphore_signal(
        barrier, inc=1, device_id=dev(p), device_id_type=pl.DeviceIdType.MESH))

    pay[0 : pn.op_rows, :] = op_ref[...]
    pay[pn.op_rows : pn.c0, :] = jnp.zeros((pn.c0 - pn.op_rows, rows), F32)
    pay[pn.c0 : pn.b0, :] = c_ref[...]
    pay[pn.b0 : pn.width, :] = jnp.zeros((pn.width - pn.b0, rows), F32)
    pay[pn.b0 : pn.tag, :] = b_ref[...]
    shift = rows.bit_length() - 1
    local = lax.bitwise_and(rrow_ref[...], rows - 1) + 1
    pay[pn.tag : pn.tag + 1, :] = local.astype(F32)

    gpart[...] = jnp.zeros(gpart.shape, F32)
    gram = jnp.zeros((k, k), F32)
    raw = jnp.zeros((1, k), F32)
    b8 = pay[pn.b0 : pn.b0 + 8, :]
    for a in range(3):
        ca = pay[pn.c0 + a * k : pn.c0 + (a + 1) * k, :]
        gram = gram + lax.dot_general(ca, ca, NT, precision=HIGH, preferred_element_type=F32)
        raw = raw + lax.dot_general(b8, ca, NT, precision=HIGH, preferred_element_type=F32)[a : a + 1]
    b3 = pay[pn.b0 : pn.tag, :]
    bb = jnp.sum(jnp.sum(b3 * b3, axis=1, keepdims=True), axis=0, keepdims=True)
    gpart[0:k, 0:k] = gram
    gpart[k : k + 1, 0:k] = raw
    gpart[k + 1 : k + 2, :] = jnp.broadcast_to(bb, (1, CZ))

    pl.semaphore_wait(barrier, peers - 1)

    def tile(t):
        return pl.ds(pl.multiple_of(t * 8, 8), 8)

    def rs_send(t, _):
        own = t * pn.stride

        @pl.when(me != own)
        def _():
            remote(gpart.at[tile(t), :], grs.at[me], rs_s.at[t], rs_r.at[me], own).start()
        return 0

    lax.fori_loop(0, pn.tiles, rs_send, 0)

    trow = lax.shift_right_logical(rrow_ref[...], shift)
    jrow = lax.broadcasted_iota(jnp.int32, (CZ, rows), 1)
    irow = lax.broadcasted_iota(jnp.int32, (CZ, rows), 0)

    diagonal = (
        lax.broadcasted_iota(jnp.int32, (CZ, CZ), 0) == lax.broadcasted_iota(jnp.int32, (CZ, CZ), 1)
    )

    def slots(i, _):
        at = pl.ds(pl.multiple_of(i * CZ, CZ), CZ)
        line = lax.shift_right_logical(rrow_ref[:, at], shift).astype(F32)
        tc = jnp.sum(jnp.where(diagonal, line, 0.0), axis=1, keepdims=True).astype(jnp.int32)
        before = jnp.logical_and(tc == trow, jrow < irow + i * CZ)
        rank = jnp.sum(jnp.where(before, 1.0, 0.0), axis=1, keepdims=True)
        slot[at, :] = jnp.broadcast_to(tc * pn.cap + rank.astype(jnp.int32), (CZ, CZ))
        return 0

    lax.fori_loop(0, rows // CZ, slots, 0)
    full = pay[...]
    hi = full.astype(BF16)
    hl[0 : pn.width, :] = hi
    hl[pn.width :, :] = (full - hi.astype(F32)).astype(BF16)

    lane = lax.broadcasted_iota(jnp.int32, (1, CZ), 1)
    block = lax.div(me, pn.per_blk)

    def spread(parts, q):
        out = None
        for j, value in enumerate(parts):
            amount = (j - q) * pn.cap % CZ
            moved = pltpu.roll(value, amount, 1) if amount else value
            out = moved if out is None else jnp.where(lane >= j * pn.cap, moved, out)
        return out

    def pack(it, _):
        gb = lax.rem(block + it, pn.nblk)
        for half in range(2):
            ids = lane + (gb * 256 + half * CZ)
            ohp[gb, :, half * CZ : (half + 1) * CZ] = jnp.where(slot[...] == ids, 1.0, 0.0).astype(BF16)
        oh = ohp[gb]
        xs[...] = jnp.dot(hl[0 : pn.width, :], oh, preferred_element_type=F32)
        xs[...] += jnp.dot(hl[pn.width :, :], oh, preferred_element_type=F32)
        for half in range(2):
            parts = [xs[j * pn.part : (j + 1) * pn.part, half * CZ : (half + 1) * CZ] for j in range(pn.fold)]
            for q in range(pn.fold):
                p = gb * pn.per_blk + half * pn.fold + q
                packet = spread(parts, q)

                @pl.when(p == me)
                def _():
                    got[p] = packet

                @pl.when(p != me)
                def _():
                    snd[p] = packet
                    remote(snd.at[p], got.at[me], bulk_s.at[p], bulk_r.at[me], p).start()
        return 0

    lax.fori_loop(0, 2, pack, 0)

    mine = lax.div(me, pn.stride)
    owner = jnp.logical_and(lax.rem(me, pn.stride) == 0, mine < pn.tiles)

    @pl.when(owner)
    def _():
        grs[me] = gpart[tile(mine), :]
        others(lambda p: remote(gpart.at[tile(0), :], grs.at[p], rs_s.at[0], rs_r.at[p], p).wait_recv())
        total = jnp.sum(grs[...], axis=0)
        gsnd[...] = total
        gfull[mine] = total
        others(lambda p: remote(gsnd, gfull.at[mine], ag_s.at[p], ag_r.at[mine], p).start())

    lax.fori_loop(2, pn.nblk, pack, 0)

    for y in range(CY):
        uv[pl.ds(y, pn.basis_rows, stride=CY), :] = u_ref[:, y * CZ : (y + 1) * CZ]
    mred[...] = jnp.zeros(mred.shape, F32)
    ginv[...] = jnp.zeros(ginv.shape, F32)

    def ag_wait(t, _):
        own = t * pn.stride

        @pl.when(me != own)
        def _():
            remote(gsnd, gfull.at[t], ag_s.at[0], ag_r.at[t], own).wait_recv()
        return 0

    lax.fori_loop(0, pn.tiles, ag_wait, 0)
    sums = gfull[...].reshape(pn.tiles * 8, CZ)
    gm[...] = sums[0:k]
    sub_k = lax.broadcasted_iota(jnp.int32, (k, 1), 0)

    def sweep(i, _):
        m = gm[...]
        row = gm[pl.ds(i, 1), :]
        at = lane == i
        col = jnp.sum(jnp.where(at, m, 0.0), axis=1, keepdims=True)
        pivot = jnp.sum(jnp.where(at, row, 0.0), axis=1, keepdims=True)
        scaled = jnp.where(at, 1.0, row) / pivot
        inner = jnp.where(at, 0.0, m) - col * scaled
        gm[...] = jnp.where(sub_k == i, scaled, inner)
        return 0

    lax.fori_loop(0, k, sweep, 0)
    ginv[0:k, :] = gm[...]

    def solve(p):
        return jnp.dot(p, ginv[...], precision=HIGH, preferred_element_type=F32)

    def bdot(p, z):
        return jnp.sum(jnp.where(lane < k, p * z, 0.0), axis=1, keepdims=True)

    s_row = jnp.broadcast_to(sums[k : k + 1, :], (8, CZ))
    bb_all = jnp.broadcast_to(sums[k + 1 : k + 2, 0:1], (8, 1))
    z0 = solve(s_row)
    beta = jnp.sqrt(bb_all - bdot(s_row, z0))

    acc[...] = jnp.zeros(acc.shape, F32)
    sub_r = lax.broadcasted_iota(jnp.int32, (rows, 1), 0).astype(F32) + 1.0

    half_n = pn.nblk // 2

    def unpack(it, _):
        far = lax.div(it, half_n)
        side = lax.rem(lax.div(block, half_n) + far, 2)
        start = jnp.where(far == 0, block, half_n - 1)
        gb = side * half_n + lax.rem(start - it + 2 * pn.nblk, half_n)
        for half in range(2):
            values = []
            for q in range(pn.fold):
                p = gb * pn.per_blk + half * pn.fold + q

                @pl.when(p != me)
                def _():
                    remote(snd.at[p], got.at[p], bulk_s.at[p], bulk_r.at[p], p).wait_recv()
            for q in range(pn.fold):
                values.append(got[gb * pn.per_blk + half * pn.fold + q])
            for j in range(pn.fold):
                xs[j * pn.part : (j + 1) * pn.part, half * CZ : (half + 1) * CZ] = spread(values, j)
            tags = xs[pn.tag : pn.tag + 1, half * CZ : (half + 1) * CZ]
            oht[gb, :, half * CZ : (half + 1) * CZ] = jnp.where(sub_r == tags, 1.0, 0.0).astype(BF16)
        x = xs[...]
        xh = x.astype(BF16)
        xhl[0 : pn.width, :] = xh
        xhl[pn.width :, :] = (x - xh.astype(F32)).astype(BF16)
        for n in range(rows // 256):
            at = slice(n * 256, (n + 1) * 256)
            o = oht[gb, at, :]
            acc[:, at] += lax.dot_general(xhl[0 : pn.width, :], o, NT, preferred_element_type=F32)
            acc[:, at] += lax.dot_general(xhl[pn.width :, :], o, NT, preferred_element_type=F32)
        return 0

    lax.fori_loop(0, pn.nblk, unpack, 0)

    def relayout(first, last):
        for y in range(CY):
            new[pl.ds(first * CY + y, last - first, stride=CY), :] = acc[first:last, y * CZ : (y + 1) * CZ]

    relayout(pn.c0, pn.width)

    def row(i):
        return new[i * CY : (i + 1) * CY, :]

    sub = lax.broadcasted_iota(jnp.int32, (CY, CZ), 0)
    lane8 = lax.broadcasted_iota(jnp.int32, (CY, CZ), 1)

    def combine(get, z):
        out = [jnp.zeros((CY, CZ), F32)] * 3
        for m in range(k):
            zb = jnp.broadcast_to(z[:, m : m + 1], (CY, CZ))
            for a in range(3):
                out[a] = out[a] + get(a * k + m) * zb
        return out

    def c_row(i):
        return row(pn.c0 + i)

    def u_row(i):
        return uv[i * CY : (i + 1) * CY, :]

    places = ((-1, 0), (1, 0), (0, 1), (-1, 1), (1, 1))

    def apply_op(phase, v, between=None):
        for b in range(3):
            hsnd[phase, b] = v[b]
        for j, (dx, oy) in enumerate(places):
            to = gx - dx
            target = to * pn.ny + (lax.rem(gy + oy, 2))

            @pl.when(jnp.logical_and(to >= 0, to < pn.nx))
            def _():
                remote(hsnd.at[phase], hrcv.at[phase, j], h_s.at[phase, j], h_r.at[phase, j], target).start()
        if between is not None:
            between()
        for j, (dx, oy) in enumerate(places):
            there = gx + dx
            source = there * pn.ny + (lax.rem(gy + oy, 2))
            valid = jnp.logical_and(there >= 0, there < pn.nx)

            @pl.when(valid)
            def _():
                remote(hsnd.at[phase], hrcv.at[phase, j], h_s.at[phase, j], h_r.at[phase, j], source).wait_recv()

            @pl.when(jnp.logical_not(valid))
            def _():
                hrcv[phase, j] = jnp.zeros((3, CY, CZ), F32)
        out = [jnp.zeros((CY, CZ), F32)] * 3
        for dx in (-1, 0, 1):
            for b in range(3):
                near = v[b] if dx == 0 else hrcv[phase, places.index((dx, 0)), b]
                side = hrcv[phase, places.index((dx, 1)), b]
                for dy in (-1, 0, 1):
                    if dy == 0:
                        moved = near
                    elif dy == -1:
                        edge = jnp.where(gy > 0, pltpu.roll(side, 1, 0), 0.0)
                        moved = jnp.where(sub == 0, edge, pltpu.roll(near, 1, 0))
                    else:
                        edge = jnp.where(gy == 0, pltpu.roll(side, CY - 1, 0), 0.0)
                        moved = jnp.where(sub == CY - 1, edge, pltpu.roll(near, CY - 1, 0))
                    for dz in (-1, 0, 1):
                        if dz == 0:
                            value = moved
                        elif dz == -1:
                            value = jnp.where(lane8 == 0, 0.0, pltpu.roll(moved, 1, 1))
                        else:
                            value = jnp.where(lane8 == CZ - 1, 0.0, pltpu.roll(moved, CZ - 1, 1))
                        kk = (dx + 1) * 9 + (dy + 1) * 3 + dz + 1
                        for a in range(3):
                            out[a] = out[a] + row((kk * 3 + a) * 3 + b) * value
        return out

    def put(i, value):
        mred[i : i + 1, :] = jnp.sum(value, axis=0, keepdims=True)

    def dot3(p, q):
        return p[0] * q[0] + p[1] * q[1] + p[2] * q[2]

    def sums_of(phase, image, vectors):
        for m in range(k):
            put(m, dot3([c_row(a * k + m) for a in range(3)], image))
        for i, vector in enumerate(vectors + [image]):
            put(k + i, dot3(vector, image))
        mine_row = lax.dot_general(jnp.ones((8, CZ), F32), mred[...], NT, precision=HIGH, preferred_element_type=F32)[0:1]
        rsnd[phase] = mine_row
        rrcv[phase, me] = mine_row
        others(lambda p: remote(rsnd.at[phase], rrcv.at[phase, me], red_s.at[phase, p], red_r.at[phase, me], p).start())
        others(lambda p: remote(rsnd.at[phase], rrcv.at[phase, p], red_s.at[phase, p], red_r.at[phase, p], p).wait_recv())
        return jnp.broadcast_to(jnp.sum(rrcv[phase], axis=0), (8, CZ))

    load = [row(pn.b0 + a) for a in range(3)]
    part = combine(c_row, z0)
    v1 = [(load[a] - part[a]) / beta for a in range(3)]
    w = apply_op(0, v1, lambda: relayout(0, pn.c0))
    p1 = sums_of(0, w, [v1])
    z1 = solve(p1)
    h11, ww = p1[:, k : k + 1], p1[:, k + 1 : k + 2]
    h21 = jnp.sqrt(ww - bdot(p1, z1) - h11 * h11)
    part = combine(c_row, z1)
    v2 = [(w[a] - part[a] - h11 * v1[a]) / h21 for a in range(3)]
    w = apply_op(1, v2)
    p2 = sums_of(1, w, [v1, v2])
    z2 = solve(p2)
    h12, h22, ww = p2[:, k : k + 1], p2[:, k + 1 : k + 2], p2[:, k + 2 : k + 3]
    h32 = jnp.sqrt(ww - bdot(p2, z2) - h12 * h12 - h22 * h22)
    m11 = h11 * h11 + h21 * h21
    m12 = h11 * h12 + h21 * h22
    m22 = h12 * h12 + h22 * h22 + h32 * h32
    g_one, g_two = beta * h11, beta * h12
    determ = m11 * m22 - m12 * m12
    y_one = (m22 * g_one - m12 * g_two) / determ
    y_two = (m11 * g_two - m12 * g_one) / determ

    ut = combine(u_row, z0 - y_one * z1 - y_two * z2)
    for y in range(CY):
        tile_y = jnp.zeros((8, CZ), F32)
        for a in range(3):
            tile_y = jnp.where(sub == a, jnp.broadcast_to(ut[a][y : y + 1, :], (8, CZ)), tile_y)
        high = tile_y.astype(BF16).astype(F32)
        ulhs[0:8, y * CZ : (y + 1) * CZ] = high
        ulhs[8:16, y * CZ : (y + 1) * CZ] = tile_y - high
    ub = ulhs[...].astype(BF16)

    def upack(gb, _):
        d = jnp.dot(ub, ohp[gb], preferred_element_type=F32)
        d = d[0:8] + d[8:16]
        usnd[2 * gb] = d[0:4, :CZ]
        usnd[2 * gb + 1] = d[0:4, CZ:]
        return 0

    lax.fori_loop(0, pn.nblk, upack, 0)
    others(lambda p: remote(usnd.at[lax.div(p, pn.fold)], urcv.at[me], u_s.at[p], u_r.at[me], p).start())
    urcv[me] = usnd[lax.div(me, pn.fold)]
    others(lambda p: remote(usnd.at[0], urcv.at[p], u_s.at[p], u_r.at[p], p).wait_recv())
    place = lax.rem(me, pn.fold)
    utmp[...] = jnp.zeros(utmp.shape, F32)

    def uunpack(gb, total):
        halves = []
        for half in range(2):
            out = None
            for q in range(pn.fold):
                at = (half * pn.fold + q) * 8
                utmp[at : at + 4, :] = urcv[gb * pn.per_blk + half * pn.fold + q]
                tile_q = utmp[at : at + 8, :]
                if pn.fold > 1:
                    tile_q = pltpu.roll(tile_q, lax.rem((q - place) * pn.cap + CZ, CZ), 1)
                out = tile_q if out is None else jnp.where(lane >= q * pn.cap, tile_q, out)
            halves.append(out)
        x = jnp.concatenate(halves, axis=1)
        high = x.astype(BF16).astype(F32)
        x2 = jnp.concatenate([high, x - high], axis=0).astype(BF16)
        return total + lax.dot_general(x2, oht[gb], NT, preferred_element_type=F32)

    moved = lax.fori_loop(0, pn.nblk, uunpack, jnp.zeros((16, rows), F32))
    moved = moved[0:8] + moved[8:16]
    sol = []
    for a in range(3):
        value = jnp.zeros((CY, CZ), F32)
        for y in range(CY):
            line = jnp.broadcast_to(moved[a : a + 1, y * CZ : (y + 1) * CZ], (CY, CZ))
            value = jnp.where(sub == y, line, value)
        sol.append(value + y_one * v1[a] + y_two * v2[a])
        sol_ref[a] = sol[a]
    w = apply_op(2, sol)
    for a in range(3):
        res_ref[a] = row(pn.b0 + a) - w[a]

    def rs_done(t, _):
        own = t * pn.stride

        @pl.when(me != own)
        def _():
            remote(gpart.at[tile(t), :], grs.at[me], rs_s.at[t], rs_r.at[me], own).wait_send()
        return 0

    lax.fori_loop(0, pn.tiles, rs_done, 0)

    @pl.when(owner)
    def _():
        others(lambda p: remote(gsnd, gfull.at[mine], ag_s.at[p], ag_r.at[mine], p).wait_send())

    others(lambda p: remote(snd.at[p], got.at[me], bulk_s.at[p], bulk_r.at[me], p).wait_send())
    for phase in range(2):
        others(lambda p: remote(rsnd.at[phase], rrcv.at[phase, me], red_s.at[phase, p], red_r.at[phase, me], p).wait_send())
    others(lambda p: remote(usnd.at[lax.div(p, pn.fold)], urcv.at[me], u_s.at[p], u_r.at[me], p).wait_send())
    for phase in range(3):
        for j, (dx, oy) in enumerate(places):
            to = gx - dx
            target = to * pn.ny + (lax.rem(gy + oy, 2))

            @pl.when(jnp.logical_and(to >= 0, to < pn.nx))
            def _():
                remote(hsnd.at[phase], hrcv.at[phase, j], h_s.at[phase, j], h_r.at[phase, j], target).wait_send()


def body(nx, ny, operator, basis_u, basis_c, right_side, new_rows):
    rows = operator.shape[1]
    pn = Plan(nx, ny, rows, operator.shape[0], basis_u.shape[0])
    n = pn.peers
    vmem, dma = pltpu.VMEM, pltpu.SemaphoreType.DMA
    out = jax.ShapeDtypeStruct((3, CY, CZ), F32)
    whole = pl.BlockSpec(memory_space=pltpu.VMEM)
    sol, res = pl.pallas_call(
        functools.partial(kernel, pn),
        out_shape=(out, out),
        in_specs=[whole] * 5,
        out_specs=(whole, whole),
        scratch_shapes=[
            vmem((pn.width, rows), F32),
            vmem((2 * pn.width, rows), BF16),
            vmem((rows, CZ), jnp.int32),
            vmem((pn.nblk, rows, 256), BF16),
            vmem((pn.width, 256), F32),
            vmem((n, pn.part, CZ), F32),
            vmem((n, pn.part, CZ), F32),
            vmem((2 * pn.width, 256), BF16),
            vmem((pn.nblk, rows, 256), BF16),
            vmem((pn.width, rows), F32),
            vmem((pn.width * CY, CZ), F32),
            vmem((pn.basis_rows * CY, CZ), F32),
            vmem((pn.tiles * 8, CZ), F32),
            vmem((n, 8, CZ), F32),
            vmem((8, CZ), F32),
            vmem((pn.tiles, 8, CZ), F32),
            vmem((pn.k, CZ), F32),
            vmem((CZ, CZ), F32),
            vmem((3, 3, CY, CZ), F32),
            vmem((3, 5, 3, CY, CZ), F32),
            vmem((CZ, CZ), F32),
            vmem((2, 1, CZ), F32),
            vmem((2, n, 1, CZ), F32),
            vmem((16, rows), F32),
            vmem((2 * pn.nblk, 4, CZ), F32),
            vmem((n, 4, CZ), F32),
            vmem((pn.per_blk * 8, CZ), F32),
            dma((n,)), dma((n,)),
            dma((pn.tiles,)), dma((n,)),
            dma((n,)), dma((pn.tiles,)),
            dma((3, 5)), dma((3, 5)),
            dma((2, n)), dma((2, n)),
            dma((n,)), dma((n,)),
        ],
        compiler_params=pltpu.CompilerParams(
            collective_id=0, has_side_effects=True, vmem_limit_bytes=60 << 20
        ),
        name="solve",
    )(operator, basis_u, basis_c, right_side, new_rows.reshape(1, rows))
    return sol.reshape(3, rows), res.reshape(3, rows)


def solution(mesh):
    split = P(None, ("gx", "gy"))
    return jax.shard_map(
        functools.partial(body, mesh.shape["gx"], mesh.shape["gy"]),
        mesh=mesh,
        in_specs=(split, split, split, split, P(("gx", "gy"))),
        out_specs=(split, split),
        check_vma=False,
    )
```
